8 devices in a mesh: dp: 1 (over z), tp: 2 (over y), fsdp: 2 (over x), cp: 2 (over core).
Axes of the slice: x: 2, y: 2, z: 1, core: 2. Of those that a mesh axis runs over, the one named last changes fastest.
Arguments:
- hidden: bfloat16 [6, 3072, 3584], P(('dp', 'fsdp'), 'cp')
- positions: int32 [6, 3072], P(('dp', 'fsdp'), 'cp')
- attn_gain: float32 [3584], replicated
- w_query: bfloat16 [3584, 28, 128], P(('fsdp', 'cp'), 'tp')
- w_key: bfloat16 [3584, 4, 128], P(('fsdp', 'cp'), 'tp')
- w_value: bfloat16 [3584, 4, 128], P(('fsdp', 'cp'), 'tp')
- w_out: bfloat16 [28, 128, 3584], P('tp', None, ('fsdp', 'cp'))
- mlp_gain: float32 [3584], replicated
- w_gate: bfloat16 [3584, 18944], P(('fsdp', 'cp'), 'tp')
- w_up: bfloat16 [3584, 18944], P(('fsdp', 'cp'), 'tp')
- w_down: bfloat16 [18944, 3584], P('tp', ('fsdp', 'cp'))
Outputs:
- output: bfloat16 [6, 3072, 3584], P(('dp', 'fsdp'), 'cp')
All inputs are finite; a program needn't handle non-finite values.
Results may differ from the reference program's by a relative error of at most 0.0123897.
Values are sent between devices in bfloat16 or wider.
A program may use at most 1 GiB of HBM per device.

```python
import numpy as np
import jax
import jax.numpy as jnp
from jax import lax

SEQS = 3
SEG_LEN = 768
CP = 2
FSDP = 2
D = 3584
HEADS = 28
KV_HEADS = 4
HEAD = 128
FF = 18944
QBLOCK = 128
ROPE_THETA = 500000.0
NORM_EPS = 1e-5
BATCH = FSDP * SEQS
SEQ = 2 * CP * SEG_LEN
GROUP = HEADS // KV_HEADS


def setup_inputs(seed: int = 0, part: int = 0) -> dict:
    part_keys = jax.random.split(jax.random.fold_in(jax.random.key(seed), part), 3)
    weight_keys = jax.random.split(jax.random.key(seed + 7919), 9)
    noise = jax.random.normal(part_keys[0], (BATCH, 2 * CP, SEG_LEN, D), jnp.float32)
    seg_mean = jax.random.normal(part_keys[1], (BATCH, 2 * CP, 1, D), jnp.float32)
    hidden = (0.6 * noise + seg_mean).reshape(BATCH, SEQ, D).astype(jnp.bfloat16)
    gaps = jax.random.randint(part_keys[2], (BATCH, SEQ), 1, 5, dtype=jnp.int32)
    true_pos = jnp.cumsum(gaps, axis=1) - 1
    seg_order = np.array([slot // 2 if slot % 2 == 0 else 2 * CP - 1 - slot // 2 for slot in range(2 * CP)])
    positions = true_pos.reshape(BATCH, 2 * CP, SEG_LEN)[:, seg_order].reshape(BATCH, SEQ).astype(jnp.int32)
    in_scale = D ** -0.5
    return {
        'hidden': hidden,
        'positions': positions,
        'attn_gain': 1.0 + 0.25 * jax.random.normal(weight_keys[0], (D,), jnp.float32),
        'w_query': (1.5 * in_scale * jax.random.normal(weight_keys[1], (D, HEADS, HEAD), jnp.float32)).astype(jnp.bfloat16),
        'w_key': (1.5 * in_scale * jax.random.normal(weight_keys[2], (D, KV_HEADS, HEAD), jnp.float32)).astype(jnp.bfloat16),
        'w_value': (in_scale * jax.random.normal(weight_keys[3], (D, KV_HEADS, HEAD), jnp.float32)).astype(jnp.bfloat16),
        'w_out': ((HEADS * HEAD) ** -0.5 * jax.random.normal(weight_keys[4], (HEADS, HEAD, D), jnp.float32)).astype(jnp.bfloat16),
        'mlp_gain': 1.0 + 0.25 * jax.random.normal(weight_keys[5], (D,), jnp.float32),
        'w_gate': (in_scale * jax.random.normal(weight_keys[6], (D, FF), jnp.float32)).astype(jnp.bfloat16),
        'w_up': (in_scale * jax.random.normal(weight_keys[7], (D, FF), jnp.float32)).astype(jnp.bfloat16),
        'w_down': (FF ** -0.5 * jax.random.normal(weight_keys[8], (FF, D), jnp.float32)).astype(jnp.bfloat16),
    }


def rms_norm(hidden_f32, gain):
    mean_sq = jnp.mean(hidden_f32 * hidden_f32, axis=-1, keepdims=True)
    return (hidden_f32 * lax.rsqrt(mean_sq + NORM_EPS) * gain).astype(jnp.bfloat16)


def rope_tables(positions):
    inv_freq = ROPE_THETA ** (-jnp.arange(0, HEAD, 2, dtype=jnp.float32) / HEAD)
    angles = positions.astype(jnp.float32)[..., None] * inv_freq
    return jnp.cos(angles)[..., None, :], jnp.sin(angles)[..., None, :]


def apply_rope(projected, rope_cos, rope_sin):
    half_dim = projected.shape[-1] // 2
    first_half = projected[..., :half_dim]
    second_half = projected[..., half_dim:]
    return jnp.concatenate([first_half * rope_cos - second_half * rope_sin, second_half * rope_cos + first_half * rope_sin], axis=-1)


def attention(queries, keys, values, positions):
    n_blocks = SEQ // QBLOCK
    q_blocks = queries.reshape(BATCH * n_blocks, QBLOCK, KV_HEADS, GROUP, HEAD)
    pos_blocks = positions.reshape(BATCH * n_blocks, QBLOCK)
    seq_ids = jnp.arange(BATCH * n_blocks) // n_blocks
    keys_f32 = keys.astype(jnp.float32)
    values_f32 = values.astype(jnp.float32)

    def one_block(block_args):
        q_blk, qpos_blk, seq_id = block_args
        k_seq = lax.dynamic_index_in_dim(keys_f32, seq_id, 0, keepdims=False)
        v_seq = lax.dynamic_index_in_dim(values_f32, seq_id, 0, keepdims=False)
        kpos_seq = lax.dynamic_index_in_dim(positions, seq_id, 0, keepdims=False)
        scores = jnp.einsum('qkgd,skd->kgqs', q_blk.astype(jnp.float32), k_seq) * (HEAD ** -0.5)
        visible = qpos_blk[:, None] >= kpos_seq[None, :]
        scores = jnp.where(visible, scores, -jnp.inf)
        row_max = jnp.max(scores, axis=-1, keepdims=True)
        probs = jnp.exp(scores - row_max)
        row_sum = jnp.sum(probs, axis=-1)
        weighted = jnp.einsum('kgqs,skd->qkgd', probs.astype(jnp.bfloat16).astype(jnp.float32), v_seq)
        return (weighted / jnp.transpose(row_sum, (2, 0, 1))[..., None]).astype(jnp.bfloat16)

    mixed = lax.map(one_block, (q_blocks, pos_blocks, seq_ids))
    return mixed.reshape(BATCH, SEQ, HEADS, HEAD)


def reference(hidden, positions, attn_gain, w_query, w_key, w_value, w_out, mlp_gain, w_gate, w_up, w_down):
    hidden_f32 = hidden.astype(jnp.float32)
    normed = rms_norm(hidden_f32, attn_gain).astype(jnp.float32)
    rope_cos, rope_sin = rope_tables(positions)
    queries = apply_rope(jnp.einsum('bsd,dhe->bshe', normed, w_query.astype(jnp.float32)), rope_cos, rope_sin).astype(jnp.bfloat16)
    keys = apply_rope(jnp.einsum('bsd,dhe->bshe', normed, w_key.astype(jnp.float32)), rope_cos, rope_sin).astype(jnp.bfloat16)
    values = jnp.einsum('bsd,dhe->bshe', normed, w_value.astype(jnp.float32)).astype(jnp.bfloat16)
    mixed = attention(queries.reshape(BATCH, SEQ, KV_HEADS, GROUP, HEAD), keys, values, positions)
    attn_out = jnp.einsum('bshe,hed->bsd', mixed.astype(jnp.float32), w_out.astype(jnp.float32)).astype(jnp.bfloat16)
    mid_resid = (hidden_f32 + attn_out.astype(jnp.float32)).astype(jnp.bfloat16)
    mid_f32 = mid_resid.astype(jnp.float32)
    normed_mlp = rms_norm(mid_f32, mlp_gain).astype(jnp.float32)
    gate_proj = jnp.einsum('bsd,df->bsf', normed_mlp, w_gate.astype(jnp.float32))
    up_proj = jnp.einsum('bsd,df->bsf', normed_mlp, w_up.astype(jnp.float32))
    act_mlp = (jax.nn.silu(gate_proj) * up_proj).astype(jnp.bfloat16)
    down_proj = jnp.einsum('bsf,fd->bsd', act_mlp.astype(jnp.float32), w_down.astype(jnp.float32)).astype(jnp.bfloat16)
    return (mid_f32 + down_proj.astype(jnp.float32)).astype(jnp.bfloat16)
```

```python
import functools

import jax
import jax.numpy as jnp
from jax import lax
from jax.experimental import pallas as pl
from jax.experimental.pallas import tpu as pltpu
from jax.sharding import PartitionSpec as P


ROPE_THETA = 500000.0
NORM_EPS = 1e-5
HEAD = 128
LOG2E = 1.4426950408889634
GROUP_AXES = ('fsdp', 'cp')
VMEM_LIMIT = 66_500_000
ROWS = 384
F_CHUNKS = (10, 10, 10, 7)
F_UNIT = 256
D_CHUNKS = ((0, 3), (3, 4))
STEPS = (
    ('q', 0), ('a', 0), ('o', 0), ('q', 1), ('q', 2), ('a', 1), ('o', 1), ('a', 2), ('n', 0), ('o', 2),
    ('g', 0, 0, 1), ('g', 0, 1, 1), ('n', 1), ('g', 1, 0, 2), ('g', 0, 2, 1), ('g', 1, 2, 1), ('R', 0), ('n', 2),
    ('g', 1, 3, 1), ('d', 1, 0, 0, 7), ('g', 2, 0, 1), ('R2', 0), ('g', 0, 3, 1),
    ('d', 1, 1, 0, 3), ('d', 0, 1, 0, 3), ('d', 0, 0, 0, 7), ('R2', 1), ('g', 2, 1, 1),
    ('d', 0, 1, 3, 4), ('d', 1, 1, 3, 4), ('g', 2, 2, 2),
    ('d', 2, 0, 0, 2), ('d', 2, 1, 0, 3), ('d', 2, 0, 2, 5), ('f', 1, 0), ('d', 2, 1, 3, 4),
    ('f', 2, 0), ('f', 0, 0), ('f', 0, 1), ('f', 1, 1), ('f', 2, 1),
)


def cost(flops, bytes_accessed):
    return pl.CostEstimate(flops=int(flops), bytes_accessed=int(bytes_accessed), transcendentals=0)


def params(n_axes):
    return pltpu.CompilerParams(dimension_semantics=('arbitrary',) * n_axes, vmem_limit_bytes=VMEM_LIMIT)


def qkv_kernel(x_ref, gain_ref, w_ref, cos_ref, sin_ref, q_ref, kv_ref, normed, *, heads, kv_heads):
    rows = x_ref.shape[1]

    def norm(i, carry):
        part = pl.ds(i * 64, 64)
        x = x_ref[0, part, :].astype(jnp.float32)
        mean_sq = jnp.mean(x * x, axis=-1, keepdims=True)
        normed[part, :] = (x * lax.rsqrt(mean_sq + NORM_EPS) * gain_ref[...]).astype(jnp.bfloat16)
        return carry

    lax.fori_loop(0, rows // 64, norm, 0)
    cos = cos_ref[...]
    sin = sin_ref[...]
    for pair in range(w_ref.shape[1] // 256):
        y = jnp.dot(normed[...], w_ref[:, pair * 256:(pair + 1) * 256], preferred_element_type=jnp.float32)
        for half in range(2):
            head = 2 * pair + half
            yh = y[:, half * HEAD:(half + 1) * HEAD]
            if head < heads + kv_heads:
                yh = yh * cos + pltpu.roll(yh, HEAD // 2, 1) * sin
            if head < heads:
                q_ref[:, head * HEAD:(head + 1) * HEAD] = yh.astype(jnp.bfloat16)
            else:
                kv_ref[:, (head - heads) * HEAD:(head - heads + 1) * HEAD] = yh.astype(jnp.bfloat16)


def qkv_project(hidden, seq, gain, w, cos, sin, heads, kv_heads, rows=512):
    _, tokens, d_model = hidden.shape
    width = w.shape[1]
    q_width, kv_width = heads * HEAD, 2 * kv_heads * HEAD
    return pl.pallas_call(
        functools.partial(qkv_kernel, heads=heads, kv_heads=kv_heads),
        out_shape=(jax.ShapeDtypeStruct((tokens, q_width), jnp.bfloat16), jax.ShapeDtypeStruct((tokens, kv_width), jnp.bfloat16)),
        grid=(tokens // rows,),
        in_specs=[
            pl.BlockSpec((1, rows, d_model), lambda i: (seq, i, 0)),
            pl.BlockSpec((1, d_model), lambda i: (0, 0)),
            pl.BlockSpec((d_model, width), lambda i: (0, 0), pipeline_mode=pl.Buffered(1)),
            pl.BlockSpec((rows, HEAD), lambda i: (seq * (tokens // rows) + i, 0)),
            pl.BlockSpec((rows, HEAD), lambda i: (seq * (tokens // rows) + i, 0)),
        ],
        out_specs=(pl.BlockSpec((rows, q_width), lambda i: (i, 0)), pl.BlockSpec((rows, kv_width), lambda i: (i, 0))),
        scratch_shapes=[pltpu.VMEM((rows, d_model), jnp.bfloat16)],
        compiler_params=params(1),
        cost_estimate=cost(2 * tokens * d_model * width, 2 * tokens * d_model),
        name='qkv_project',
    )(hidden, gain, w, cos, sin)


def attn_kernel(place_ref, q_ref, k_mine, v_mine, k_peer, v_peer, o_ref, m_scr, l_scr, acc_scr, k_ref, v_ref, *, heads, seg_len, scale):
    step = pl.program_id(1)
    cp = place_ref[0]
    slot = (step >= 1 + cp).astype(jnp.int32)
    seg = step - slot * (1 + cp)
    diagonal = (step == cp) | (step == 4)
    mine = ((seg == 1) | (seg == 2)).astype(jnp.int32) == cp
    k_ref[...] = jnp.where(mine, k_mine[...], k_peer[...])
    v_ref[...] = jnp.where(mine, v_mine[...], v_peer[...])

    @pl.when(seg == 0)
    def _():
        m_scr[...] = jnp.full_like(m_scr, -jnp.inf)
        l_scr[...] = jnp.zeros_like(l_scr)
        acc_scr[...] = jnp.zeros_like(acc_scr)

    def score(h, i, width, last):
        rs = slice(i * ROWS, (i + 1) * ROWS)
        hs = slice(h * HEAD, (h + 1) * HEAD)
        return lax.dot_general(q_ref[rs, hs], k_ref[0:width, :], (((1,), (1,)), ((), ())), preferred_element_type=jnp.float32)

    def absorb(s, h, i, width, last):
        rs = slice(i * ROWS, (i + 1) * ROWS)
        hs = slice(h * HEAD, (h + 1) * HEAD)
        if last:
            row = lax.broadcasted_iota(jnp.int32, (ROWS, width), 0) + i * ROWS
            col = lax.broadcasted_iota(jnp.int32, (ROWS, width), 1)
            s = jnp.where(col <= row, s, -jnp.inf)
        m_old = m_scr[h, rs, :]
        m_new = jnp.maximum(m_old, jnp.max(s, axis=1, keepdims=True))
        alpha = jnp.exp2((m_old - m_new) * scale)
        p = jnp.exp2((s - m_new[:, :1]) * scale)
        l_new = alpha * l_scr[h, rs, :] + jnp.sum(p, axis=1, keepdims=True)
        pv = jnp.dot(p.astype(jnp.bfloat16), v_ref[0:width, :], preferred_element_type=jnp.float32)
        acc = alpha * acc_scr[rs, hs] + pv
        if last:
            o_ref[rs, hs] = (acc / l_new).astype(jnp.bfloat16)
        else:
            m_scr[h, rs, :] = m_new
            l_scr[h, rs, :] = l_new
            acc_scr[rs, hs] = acc

    def run(tiles):
        ahead = score(*tiles[0])
        for n, tile in enumerate(tiles):
            s, ahead = ahead, score(*tiles[n + 1]) if n + 1 < len(tiles) else None
            absorb(s, *tile)

    blocks = [(h, i) for h in range(heads) for i in range(seg_len // ROWS)]

    @pl.when(jnp.logical_not(diagonal))
    def _():
        run([(h, i, seg_len, False) for h, i in blocks])

    @pl.when(diagonal)
    def _():
        run([(h, i, (i + 1) * ROWS, True) for h, i in blocks])


def attention(place, q, kv, kv_peer, kv_heads):
    tokens, width = q.shape
    seg_len = tokens // 2
    group_width = width // kv_heads
    heads = group_width // HEAD

    def slot_of(step, c):
        return (step >= 1 + c).astype(jnp.int32)

    def kv_map(offset):
        def index(g, step, place):
            seg = step - slot_of(step, place[0]) * (1 + place[0])
            return seg // 2, offset + g

        return index

    q_spec = pl.BlockSpec((seg_len, group_width), lambda g, step, place: (slot_of(step, place[0]), g))
    k_spec = pl.BlockSpec((seg_len, HEAD), kv_map(0))
    v_spec = pl.BlockSpec((seg_len, HEAD), kv_map(kv_heads))
    return pl.pallas_call(
        functools.partial(attn_kernel, heads=heads, seg_len=seg_len, scale=HEAD ** -0.5 * LOG2E),
        out_shape=jax.ShapeDtypeStruct((tokens, width), jnp.bfloat16),
        grid_spec=pltpu.PrefetchScalarGridSpec(
            num_scalar_prefetch=1,
            grid=(kv_heads, 5),
            in_specs=[q_spec, k_spec, v_spec, k_spec, v_spec],
            out_specs=q_spec,
            scratch_shapes=[
                pltpu.VMEM((heads, seg_len, HEAD), jnp.float32),
                pltpu.VMEM((heads, seg_len, HEAD), jnp.float32),
                pltpu.VMEM((seg_len, group_width), jnp.float32),
                pltpu.VMEM((seg_len, HEAD), jnp.bfloat16),
                pltpu.VMEM((seg_len, HEAD), jnp.bfloat16),
            ],
        ),
        compiler_params=params(2),
        cost_estimate=cost(18 * width * seg_len * seg_len, 4 * tokens * width),
        name='attention',
    )(place, q, kv, kv, kv_peer, kv_peer)


def resid_norm_kernel(h_ref, part_ref, peer_ref, gain_ref, r_ref, b_ref):
    attn = (part_ref[...].astype(jnp.float32) + peer_ref[...].astype(jnp.float32)).astype(jnp.bfloat16)
    r16 = (h_ref[0].astype(jnp.float32) + attn.astype(jnp.float32)).astype(jnp.bfloat16)
    r_ref[...] = r16
    r = r16.astype(jnp.float32)
    mean_sq = jnp.mean(r * r, axis=-1, keepdims=True)
    b_ref[...] = (r * lax.rsqrt(mean_sq + NORM_EPS) * gain_ref[...]).astype(jnp.bfloat16)


def resid_norm(hidden, seq, part, peer, gain, rows=256):
    tokens, d_model = part.shape
    block = pl.BlockSpec((rows, d_model), lambda i: (i, 0))
    return pl.pallas_call(
        resid_norm_kernel,
        out_shape=(jax.ShapeDtypeStruct((tokens, d_model), jnp.bfloat16),) * 2,
        grid=(tokens // rows,),
        in_specs=[pl.BlockSpec((1, rows, d_model), lambda i: (seq, i, 0)), block, block, pl.BlockSpec((1, d_model), lambda i: (0, 0))],
        out_specs=(block, block),
        compiler_params=params(1),
        cost_estimate=cost(10 * tokens * d_model, 10 * tokens * d_model),
        name='resid_norm',
    )(hidden, part, peer, gain)


def gate_up_kernel(b_ref, *refs, blocks):
    u_ref = refs[-1]
    step = pl.program_id(0)
    at = 0
    for k, n in enumerate(blocks):
        @pl.when((step >= at) & (step < at + n))
        def _(wg_ref=refs[2 * k], wu_ref=refs[2 * k + 1]):
            g = jnp.dot(b_ref[...], wg_ref[...], preferred_element_type=jnp.float32)
            t = jnp.dot(b_ref[...], wu_ref[...], preferred_element_type=jnp.float32)
            u_ref[...] = (jax.nn.silu(g) * t).astype(jnp.bfloat16)

        at += n


def gate_up(b, weights, u, first, ff):
    tokens, d_model = b.shape
    blocks = tuple(w.shape[1] // (2 * F_UNIT) for w in weights)
    in_specs = [pl.BlockSpec((tokens, d_model), lambda j: (0, 0), pipeline_mode=pl.Buffered(1))]
    operands = [b]
    at = 0
    for w, n in zip(weights, blocks):
        for side in (0, n):
            in_specs.append(pl.BlockSpec((d_model, F_UNIT), lambda j, at=at, n=n, side=side: (0, side + jnp.clip(j - at, 0, n - 1))))
            operands.append(w)
        at += n
    aliases = {}
    if u is not None:
        aliases = {len(operands): 0}
        in_specs.append(pl.BlockSpec(memory_space=pl.ANY))
        operands.append(u)
    return pl.pallas_call(
        functools.partial(gate_up_kernel, blocks=blocks),
        out_shape=jax.ShapeDtypeStruct((tokens, ff), jnp.bfloat16),
        grid=(sum(blocks),),
        in_specs=in_specs,
        out_specs=pl.BlockSpec((tokens, F_UNIT), lambda j: (0, first + j)),
        input_output_aliases=aliases,
        compiler_params=params(1),
        cost_estimate=cost(4 * tokens * d_model * sum(blocks) * F_UNIT, 4 * d_model * sum(blocks) * F_UNIT),
        name='gate_up',
    )(*operands)


def down_kernel(u_ref, w0_ref, w1_ref, o_ref):
    w = jnp.concatenate([w0_ref[...], w1_ref[...]], axis=1)
    y = jnp.dot(u_ref[...], w, preferred_element_type=jnp.float32).astype(jnp.bfloat16)
    o_ref[0] = y[:, :HEAD]
    o_ref[1] = y[:, HEAD:]


def down_project(u, w0, w1, first, blocks, rows=768):
    tokens, ff = u.shape
    w_spec = pl.BlockSpec((ff, HEAD), lambda i, j: (0, first + j))
    return pl.pallas_call(
        down_kernel,
        out_shape=jax.ShapeDtypeStruct((2, tokens, blocks * HEAD), jnp.bfloat16),
        grid=(tokens // rows, blocks),
        in_specs=[pl.BlockSpec((rows, ff), lambda i, j: (i, 0)), w_spec, w_spec],
        out_specs=pl.BlockSpec((2, rows, HEAD), lambda i, j: (0, i, j)),
        compiler_params=params(2),
        cost_estimate=cost(4 * tokens * ff * blocks * HEAD, 2 * tokens * ff),
        name='down_project',
    )(u, w0, w1)


def final_kernel(place_ref, r_ref, *refs):
    n = sum(ref.shape[0] == 2 for ref in refs[:-1]) // 2
    out_ref = refs[-1]
    cp = place_ref[0]
    shard = r_ref.shape[1] // 2
    for side in range(2):
        at = side * shard
        for part_ref, peer_ref in zip(refs[:n], refs[n:2 * n]):
            width = part_ref.shape[2]
            down = (part_ref[cp ^ side].astype(jnp.float32) + peer_ref[cp ^ side].astype(jnp.float32)).astype(jnp.bfloat16)
            cs = slice(at, at + width)
            out_ref[0, :, cs] = (r_ref[:, cs].astype(jnp.float32) + down.astype(jnp.float32)).astype(jnp.bfloat16)
            at += width


def final_add(place, r, parts, peers, out, seq, half, shape, rows=768):
    tokens, d_model = r.shape
    width = d_model // 2
    piece_specs = [pl.BlockSpec((2, rows, p.shape[2]), lambda i, place: (0, i, 0)) for p in parts]
    in_specs = [pl.BlockSpec((rows, width), lambda i, place: (i, place[1] ^ half))] + piece_specs + piece_specs
    operands = [r, *parts, *peers]
    aliases = {}
    if out is not None:
        in_specs.append(pl.BlockSpec(memory_space=pl.ANY))
        operands.append(out)
        aliases = {len(operands): 0}
    return pl.pallas_call(
        final_kernel,
        out_shape=jax.ShapeDtypeStruct(shape, jnp.bfloat16),
        grid_spec=pltpu.PrefetchScalarGridSpec(
            num_scalar_prefetch=1,
            grid=(tokens // rows,),
            in_specs=in_specs,
            out_specs=pl.BlockSpec((1, rows, width), lambda i, place: (seq, i, place[1] ^ half)),
        ),
        input_output_aliases=aliases,
        compiler_params=params(1),
        cost_estimate=cost(3 * tokens * width, 10 * tokens * width),
        name='final_add',
    )(place, *operands)


def after(value, *earlier):
    return lax.optimization_barrier((value, *earlier))[0]


def solution(mesh):
    seq_spec = P(('dp', 'fsdp'), 'cp', None)
    pos_spec = P(('dp', 'fsdp'), 'cp')
    in_spec = P(GROUP_AXES, 'tp', None)
    out_spec = P('tp', None, GROUP_AXES)
    col_spec = P(GROUP_AXES, 'tp')
    row_spec = P('tp', GROUP_AXES)
    rep_spec = P(None)
    swap = [(0, 1), (1, 0)]

    def layer_local(hidden, positions, attn_gain, w_query, w_key, w_value, w_out, mlp_gain, w_gate, w_up, w_down):
        n_seqs, _, _ = hidden.shape
        heads, kv_heads = w_query.shape[1], w_key.shape[1]
        shard = w_query.shape[0]
        ff = w_gate.shape[1]

        w_qkv = jnp.concatenate([w.reshape(shard, -1) for w in (w_query, w_key, w_value)], axis=1)
        full_qkv = lax.all_gather(w_qkv, GROUP_AXES, axis=0, tiled=True)
        full_out = lax.all_gather(w_out.reshape(heads * HEAD, shard), GROUP_AXES, axis=1, tiled=True)
        full_gu, firsts, at = [], [], 0
        for n in F_CHUNKS:
            cs = slice(at * F_UNIT, (at + n) * F_UNIT)
            firsts.append(at)
            chunk = jnp.concatenate([w_gate[:, cs], w_up[:, cs]], axis=1)
            full_gu.append(lax.all_gather(chunk, GROUP_AXES, axis=0, tiled=True))
            at += n
        down_local = (w_down, lax.ppermute(w_down, 'cp', swap))
        own_chunks = [w_down[:, first * HEAD:(first + n) * HEAD] for first, n in D_CHUNKS]
        remote, down_remote = [], {}

        inv_freq = ROPE_THETA ** (-jnp.arange(0, HEAD, 2, dtype=jnp.float32) / HEAD)
        angles = positions.reshape(-1).astype(jnp.float32)[:, None] * inv_freq
        cos, sin = jnp.cos(angles), jnp.sin(angles)
        cos = jnp.concatenate([cos, cos], axis=-1)
        sin = jnp.concatenate([-sin, sin], axis=-1)
        place = jnp.stack([lax.axis_index('cp'), lax.axis_index('fsdp')]).astype(jnp.int32)

        q, kv, kv_peer, part, peer, r, b, u = ([None] * n_seqs for _ in range(8))
        d_part = {(s, half): [] for s in range(n_seqs) for half in range(2)}
        d_peer = {key: [] for key in d_part}
        out, last = None, own_chunks[0]

        def tied(value):
            return after(value, last)

        for kind, s, *rest in STEPS:
            if kind == 'q':
                q[s], kv[s] = qkv_project(tied(hidden), s, attn_gain[None], full_qkv, cos, sin, heads, kv_heads)
                last = kv[s]
            elif kind == 'a':
                last = attention(place, tied(q[s]), kv[s], kv_peer[s], kv_heads)
                part[s] = last
            elif kind == 'o':
                last = jnp.dot(tied(part[s]), full_out, preferred_element_type=jnp.float32).astype(jnp.bfloat16)
                part[s] = last
            elif kind == 'n':
                r[s], b[s] = resid_norm(hidden, s, tied(part[s]), peer[s], mlp_gain[None])
                last = b[s]
            elif kind == 'g':
                c, n = rest
                last = u[s] = gate_up(tied(b[s]), full_gu[c:c + n], u[s], firsts[c], ff)
            elif kind == 'd':
                half, first, n = rest
                if half:
                    last = down_project(tied(u[s]), *down_remote[first, n], 0, n)
                else:
                    last = down_project(tied(u[s]), *down_local, first, n)
                d_part[s, half].append(last)
            elif kind == 'f':
                half = rest[0]
                last = out = final_add(place, r[s], [tied(p) for p in d_part[s, half]], d_peer[s, half], out, s, half, hidden.shape)
            if kind == 'R':
                for chunk, columns in enumerate(own_chunks):
                    remote.append(lax.ppermute(tied(columns), 'fsdp', swap))
            if kind == 'R2':
                down_remote[D_CHUNKS[s]] = (remote[s], lax.ppermute(tied(remote[s]), 'cp', swap))
            if kind == 'q':
                kv_peer[s] = lax.ppermute(kv[s], 'cp', swap)
            elif kind == 'o':
                peer[s] = lax.ppermute(part[s], 'tp', swap)
            elif kind == 'd':
                d_peer[s, half].append(lax.ppermute(last, 'tp', swap))
        return out

    return jax.shard_map(layer_local, mesh=mesh, in_specs=(seq_spec, pos_spec, rep_spec, in_spec, in_spec, in_spec, out_spec, rep_spec, col_spec, col_spec, row_spec), out_specs=seq_spec, check_vma=False)
```
